128 devices in a mesh: dp: 1, sp: 64 (over z, y, x), tp: 2 (over core).
Axes of the slice: x: 4, y: 4, z: 4, core: 2. Of those that a mesh axis runs over, the one named last changes fastest.
Arguments:
- x: bfloat16 [8192, 2048], P(('dp', 'sp', 'tp'))
- segment_ids: int32 [8192], P(('dp', 'sp', 'tp'))
- positions: int32 [8192], P(('dp', 'sp', 'tp'))
- g_attn: bfloat16 [6, 2048], replicated
- w_q: bfloat16 [6, 2048, 16, 128], P(None, None, 'tp')
- w_k: bfloat16 [6, 2048, 2, 128], replicated
- w_v: bfloat16 [6, 2048, 2, 128], replicated
- w_o: bfloat16 [6, 16, 128, 2048], P(None, 'tp')
- g_mlp: bfloat16 [6, 2048], replicated
- w_gate: bfloat16 [6, 2048, 11008], P(None, None, 'tp')
- w_up: bfloat16 [6, 2048, 11008], P(None, None, 'tp')
- w_down: bfloat16 [6, 11008, 2048], P(None, 'tp')
Outputs:
- output: bfloat16 [8192, 2048], P(('dp', 'sp', 'tp'))
All inputs are finite; a program needn't handle non-finite values.
Results may differ from the reference program's by a relative error of at most 0.02.
Values are sent between devices in bfloat16 or wider.
A program may use at most 1.5 GiB of HBM per device.

```python
import jax
import jax.numpy as jnp
from jax import lax

D = 2048
HEADS = 16
KV_HEADS = 2
HEAD = 128
FF = 11008
LAYERS = 6
TOKENS = 8192
WINDOW = 1024
ROPE_BASE = 10000
EPS = 1e-6
REF_ROWS = max(1024 // HEADS, 8)
GROUP = HEADS // KV_HEADS


def draw_layout(layout_key):
    k_first, k_second, k_step, k_offset = jax.random.split(layout_key, 4)
    first_cut = jax.random.randint(k_first, (), TOKENS // 2, 3 * TOKENS // 4)
    second_cut = jax.random.randint(k_second, (), first_cut + TOKENS // 16, TOKENS - TOKENS // 16 + 1)
    tok_index = jnp.arange(TOKENS)
    segment_ids = (tok_index >= first_cut).astype(jnp.int32) + (tok_index >= second_cut).astype(jnp.int32)
    step_sizes = jax.random.randint(k_step, (TOKENS,), 1, 8)
    before = jnp.cumsum(step_sizes) - step_sizes
    seg_starts = before[jnp.stack([jnp.zeros((), first_cut.dtype), first_cut, second_cut])]
    seg_offsets = jax.random.randint(k_offset, (3,), 0, 512)
    positions = before - seg_starts[segment_ids] + seg_offsets[segment_ids]
    return segment_ids, positions.astype(jnp.int32)


def draw_stack(stack_key, shape, scale):
    layer_keys = jax.random.split(stack_key, LAYERS)
    return lax.map(lambda one_key: (jax.random.normal(one_key, shape, jnp.float32) * scale).astype(jnp.bfloat16), layer_keys)


def setup_inputs(seed: int = 0, part: int = 0) -> dict:
    root_key = jax.random.key(seed)
    part_key = jax.random.fold_in(root_key, part)
    k_layout, k_noise, k_walk = jax.random.split(part_key, 3)
    segment_ids, positions = draw_layout(k_layout)
    noise = jax.random.normal(k_noise, (TOKENS, D), jnp.float32)
    walk = jnp.cumsum(jax.random.normal(k_walk, (TOKENS, D), jnp.float32), axis=0) * (1.5 / TOKENS ** 0.5)
    x = (0.6 * noise + walk).astype(jnp.bfloat16)
    w_keys = jax.random.split(jax.random.key(seed + 1), 8)
    gains = 1.0 + 0.5 * jax.random.normal(w_keys[0], (2, LAYERS, D), jnp.float32)
    return {
        "x": x,
        "segment_ids": segment_ids,
        "positions": positions,
        "g_attn": gains[0].astype(jnp.bfloat16),
        "w_q": draw_stack(w_keys[1], (D, HEADS, HEAD), D ** -0.5),
        "w_k": draw_stack(w_keys[2], (D, KV_HEADS, HEAD), D ** -0.5),
        "w_v": draw_stack(w_keys[3], (D, KV_HEADS, HEAD), D ** -0.5),
        "w_o": draw_stack(w_keys[4], (HEADS, HEAD, D), (HEADS * HEAD) ** -0.5),
        "g_mlp": gains[1].astype(jnp.bfloat16),
        "w_gate": draw_stack(w_keys[5], (D, FF), D ** -0.5),
        "w_up": draw_stack(w_keys[6], (D, FF), D ** -0.5),
        "w_down": draw_stack(w_keys[7], (FF, D), FF ** -0.5),
    }


def rms_norm(x, gain):
    x_wide = x.astype(jnp.float32)
    inv_rms = lax.rsqrt(jnp.mean(x_wide * x_wide, axis=-1, keepdims=True) + EPS)
    return (x_wide * inv_rms * gain.astype(jnp.float32)).astype(jnp.bfloat16)


def rope(t, cos_tab, sin_tab):
    half_width = HEAD // 2
    t_wide = t.astype(jnp.float32)
    lower_half = t_wide[..., :half_width]
    upper_half = t_wide[..., half_width:]
    return jnp.concatenate([lower_half * cos_tab - upper_half * sin_tab, upper_half * cos_tab + lower_half * sin_tab], axis=-1).astype(jnp.bfloat16)


def attention(q, k, v, segment_ids, windowed):
    block_rows = REF_ROWS
    key_span = min(block_rows + WINDOW, TOKENS) if windowed else TOKENS
    blocks = TOKENS // block_rows
    q_blocks = q.reshape(blocks, block_rows, KV_HEADS, GROUP, HEAD)

    def one_block(block_args):
        q_blk, block_idx = block_args
        q_start = block_idx * block_rows
        k_start = jnp.clip(q_start + block_rows - key_span, 0, TOKENS - key_span)
        k_blk = lax.dynamic_slice_in_dim(k, k_start, key_span, 0)
        v_blk = lax.dynamic_slice_in_dim(v, k_start, key_span, 0)
        seg_q = lax.dynamic_slice_in_dim(segment_ids, q_start, block_rows, 0)
        seg_k = lax.dynamic_slice_in_dim(segment_ids, k_start, key_span, 0)
        q_pos = q_start + jnp.arange(block_rows)
        k_pos = k_start + jnp.arange(key_span)
        allowed = (k_pos[None, :] <= q_pos[:, None]) & (seg_k[None, :] == seg_q[:, None])
        if windowed:
            allowed = allowed & (q_pos[:, None] - k_pos[None, :] < WINDOW)
        scores = jnp.einsum("qgrd,kgd->qgrk", q_blk.astype(jnp.float32), k_blk.astype(jnp.float32)) * HEAD ** -0.5
        scores = jnp.where(allowed[:, None, None, :], scores, -1e30)
        attn_probs = jax.nn.softmax(scores, axis=-1).astype(jnp.bfloat16).astype(jnp.float32)
        mixed = jnp.einsum("qgrk,kgd->qgrd", attn_probs, v_blk.astype(jnp.float32))
        return mixed.astype(jnp.bfloat16)

    out_blocks = lax.map(one_block, (q_blocks, jnp.arange(blocks)))
    return out_blocks.reshape(TOKENS, HEADS * HEAD)


def decoder_layer(x, params, cos_tab, sin_tab, segment_ids, windowed):
    g_attn, w_q, w_k, w_v, w_o, g_mlp, w_gate, w_up, w_down = params
    normed = rms_norm(x, g_attn)
    q = jnp.dot(normed, w_q.reshape(D, HEADS * HEAD), preferred_element_type=jnp.float32).astype(jnp.bfloat16)
    k = jnp.dot(normed, w_k.reshape(D, KV_HEADS * HEAD), preferred_element_type=jnp.float32).astype(jnp.bfloat16)
    v = jnp.dot(normed, w_v.reshape(D, KV_HEADS * HEAD), preferred_element_type=jnp.float32).astype(jnp.bfloat16)
    q = rope(q.reshape(TOKENS, HEADS, HEAD), cos_tab, sin_tab).reshape(TOKENS, KV_HEADS, GROUP, HEAD)
    k = rope(k.reshape(TOKENS, KV_HEADS, HEAD), cos_tab, sin_tab)
    v = v.reshape(TOKENS, KV_HEADS, HEAD)
    mixed = attention(q, k, v, segment_ids, windowed)
    attn_out = jnp.dot(mixed, w_o.reshape(HEADS * HEAD, D), preferred_element_type=jnp.float32).astype(jnp.bfloat16)
    hidden = (x.astype(jnp.float32) + attn_out.astype(jnp.float32)).astype(jnp.bfloat16)
    normed = rms_norm(hidden, g_mlp)
    gate_proj = jnp.dot(normed, w_gate, preferred_element_type=jnp.float32)
    up_proj = jnp.dot(normed, w_up, preferred_element_type=jnp.float32)
    activation = (jax.nn.silu(gate_proj) * up_proj).astype(jnp.bfloat16)
    mlp_out = jnp.dot(activation, w_down, preferred_element_type=jnp.float32).astype(jnp.bfloat16)
    return (hidden.astype(jnp.float32) + mlp_out.astype(jnp.float32)).astype(jnp.bfloat16)


def reference(x, segment_ids, positions, g_attn, w_q, w_k, w_v, w_o, g_mlp, w_gate, w_up, w_down):
    inv_freq = ROPE_BASE ** (-jnp.arange(HEAD // 2, dtype=jnp.float32) / (HEAD // 2))
    angles = positions.astype(jnp.float32)[:, None] * inv_freq[None, :]
    cos_tab = jnp.cos(angles)[:, None, :]
    sin_tab = jnp.sin(angles)[:, None, :]
    stacked = tuple(w.reshape((LAYERS // 2, 2) + w.shape[1:]) for w in (g_attn, w_q, w_k, w_v, w_o, g_mlp, w_gate, w_up, w_down))

    def pair_step(residual, layer_pair):
        residual = decoder_layer(residual, tuple(w[0] for w in layer_pair), cos_tab, sin_tab, segment_ids, True)
        residual = decoder_layer(residual, tuple(w[1] for w in layer_pair), cos_tab, sin_tab, segment_ids, False)
        return residual, None

    final_x, unused_ys = lax.scan(pair_step, x, stacked)
    return final_x
```

```python
import functools
import math

import jax
import jax.numpy as jnp
from jax import lax
from jax.experimental import pallas as pl
from jax.experimental.pallas import tpu as pltpu
from jax.sharding import PartitionSpec as P

EPS = 1e-6
ROPE_BASE = 10000.0
WINDOW = 1024
NEG = -1e30
MESH = pl.DeviceIdType.MESH
F32 = jnp.float32
BF16 = jnp.bfloat16
K_CUTS = (48, 48, 32)
V_CUTS = (32, 48, 48)
STRIDES = (1, 4, 16)
ORDERS = ((0, 1, 2), (1, 2, 0), (2, 0, 1))


def dot(a, b):
    return jnp.dot(a, b, preferred_element_type=F32)


def rms_norm(x, gain):
    x_wide = x.astype(F32)
    inv_rms = lax.rsqrt(jnp.mean(x_wide * x_wide, axis=-1, keepdims=True) + EPS)
    return (x_wide * inv_rms * gain.astype(F32)).astype(BF16)


def rope_tables(positions, head_dim):
    half_width = head_dim // 2
    inv_freq = ROPE_BASE ** (-jnp.arange(half_width, dtype=F32) / half_width)
    angles = positions.astype(F32)[:, None] * inv_freq[None, :]
    return jnp.cos(angles)[:, None, :], jnp.sin(angles)[:, None, :]


def rope(t, cos_tab, sin_tab):
    half_width = t.shape[-1] // 2
    t_wide = t.astype(F32)
    lower_half = t_wide[..., :half_width]
    upper_half = t_wide[..., half_width:]
    return jnp.concatenate([lower_half * cos_tab - upper_half * sin_tab, upper_half * cos_tab + lower_half * sin_tab], axis=-1).astype(BF16)


def build_queries(q_ref, cuts_ref, q_ext, q_base, heads, rows, hd):
    for h in range(heads):
        q_ext[0:hd, h * rows:(h + 1) * rows] = q_ref[:, h * hd:(h + 1) * hd].astype(F32).T.astype(BF16)
    cut0 = cuts_ref[0:1, :]
    cut1 = cuts_ref[1:2, :]
    q_pos = q_base + lax.broadcasted_iota(jnp.int32, (hd, rows), 1)
    seg_q = (q_pos >= cut0).astype(jnp.int32) + (q_pos >= cut1).astype(jnp.int32)
    feat = lax.broadcasted_iota(jnp.int32, (hd, rows), 0)
    val = jnp.where((feat < 4) & (feat != seg_q), NEG, 0.0).astype(BF16)
    for h in range(heads):
        q_ext[hd:2 * hd, h * rows:(h + 1) * rows] = val


def key_features(cuts_ref, k_base, keys, hd):
    cut0 = cuts_ref[0:1, :]
    cut1 = cuts_ref[1:2, :]
    k_pos = k_base + lax.broadcasted_iota(jnp.int32, (keys, hd), 0)
    seg_k = (k_pos >= cut0).astype(jnp.int32) + (k_pos >= cut1).astype(jnp.int32)
    seg_k = jnp.where(k_pos < 0, 3, seg_k)
    feat = lax.broadcasted_iota(jnp.int32, (keys, hd), 1)
    return jnp.where(feat == seg_k, 1.0, 0.0).astype(BF16)


def attend_tile(k, v_t, cuts_ref, q_ext, acc, m_ref, l_ref, k_base, q_base, rows, causal, windowed):
    keys, hd = k.shape
    cols = q_ext.shape[1]
    feats = key_features(cuts_ref, k_base, keys, hd)
    k_ext = jnp.concatenate([k, feats], axis=1)
    scale = math.log2(math.e) * hd ** -0.5
    s = dot(k_ext, q_ext[...])
    if causal or windowed:
        k_pos = k_base + lax.broadcasted_iota(jnp.int32, (keys, rows), 0)
        q_pos = q_base + lax.broadcasted_iota(jnp.int32, (keys, rows), 1)
        ok = (k_pos <= q_pos) if causal else (q_pos - k_pos < WINDOW)
        bias = jnp.where(ok, 0.0, NEG)
        s = jnp.concatenate([s[:, h * rows:(h + 1) * rows] + bias for h in range(cols // rows)], axis=1)
    m_prev = m_ref[...]
    m_new = jnp.maximum(m_prev, jnp.max(s, axis=0, keepdims=True))
    p = jnp.exp2((s - m_new) * scale)
    alpha = jnp.exp2((m_prev - m_new) * scale)
    m_ref[...] = m_new
    l_ref[...] = l_ref[...] * alpha + jnp.sum(p, axis=0, keepdims=True)
    acc[...] = acc[...] * alpha + dot(v_t, p.astype(BF16))


def start_state(acc, m_ref, l_ref):
    acc[...] = jnp.zeros_like(acc)
    m_ref[...] = jnp.full_like(m_ref, -3e37)
    l_ref[...] = jnp.zeros_like(l_ref)


def finish_state(mixed_ref, acc, l_ref, heads, rows, hd):
    inv = 1.0 / l_ref[...]
    for h in range(heads):
        cols = slice(h * rows, (h + 1) * rows)
        mixed_ref[:, h * hd:(h + 1) * hd] = (acc[:, cols] * inv[:, cols]).T.astype(BF16)


def window_kernel(sp_size, back, q_ref, kv_ref, cuts_ref, mixed_ref, buf, q_ext, acc, m_ref, l_ref, send_sem, recv_sem):
    rows, width = q_ref.shape
    hd = kv_ref.shape[1]
    heads = width // hd
    me = lax.axis_index("sp")
    barrier = pltpu.get_barrier_semaphore()
    for d in range(1, back + 1):
        pl.semaphore_signal(barrier, inc=1, device_id={"sp": lax.rem(me - d + sp_size, sp_size)}, device_id_type=MESH)
    pl.semaphore_wait(barrier, back)
    copies = []
    for d in range(1, back + 1):
        cp = pltpu.make_async_remote_copy(kv_ref, buf.at[back - d], send_sem.at[d - 1], recv_sem.at[back - d], device_id={"sp": lax.rem(me + d, sp_size)}, device_id_type=MESH)
        cp.start()
        copies.append(cp)
    q_base = me * rows
    build_queries(q_ref, cuts_ref, q_ext, q_base, heads, rows, hd)
    start_state(acc, m_ref, l_ref)
    attend_tile(kv_ref[0:rows, :], kv_ref[rows:2 * rows, :], cuts_ref, q_ext, acc, m_ref, l_ref, q_base, q_base, rows, True, False)
    per = 4
    for t in reversed(range(back // per)):
        for j in range(per):
            slot = t * per + j
            copies[back - slot - 1].wait_recv()
        k = jnp.concatenate([buf[t * per + j, 0:rows, :] for j in range(per)], axis=0)
        v_t = jnp.concatenate([buf[t * per + j, rows:2 * rows, :] for j in range(per)], axis=1)
        attend_tile(k, v_t, cuts_ref, q_ext, acc, m_ref, l_ref, q_base + (t * per - back) * rows, q_base, rows, False, t == 0)
    finish_state(mixed_ref, acc, l_ref, heads, rows, hd)
    for cp in copies:
        cp.wait_send()


def global_kernel(q_ref, kv_ref, cuts_ref, mixed_ref, buf_a, buf_b, buf_c, q_ext, acc, m_ref, l_ref, send_sem, recv_sem, own_sem):
    rows, width = q_ref.shape
    hd = kv_ref.shape[1]
    heads = width // hd
    me = lax.axis_index("sp")
    coords = (lax.rem(me, 4), lax.rem(me // 4, 4), me // 16)
    bufs = (buf_a, buf_b, buf_c)

    def peer(axis, step):
        c = coords[axis]
        return {"sp": me + (lax.rem(c + step + 4, 4) - c) * STRIDES[axis]}

    barrier = pltpu.get_barrier_semaphore()
    for axis in range(3):
        for step in (1, -1):
            pl.semaphore_signal(barrier, inc=1, device_id=peer(axis, step), device_id_type=MESH)
    offset = 0
    for o, (k_rows, v_rows) in enumerate(zip(K_CUTS, V_CUTS)):
        a1, a2, a3 = ORDERS[o]
        bufs[o][coords[a3], coords[a2], coords[a1]] = kv_ref[offset:offset + k_rows + v_rows, :]
        offset += k_rows + v_rows
    pl.semaphore_wait(barrier, 6)

    def part(o, phase, c, half):
        a1, a2, a3 = ORDERS[o]
        if phase == 0:
            cut = 48
            r = pl.ds(0, cut) if half == 0 else pl.ds(cut, K_CUTS[o] + V_CUTS[o] - cut)
            return bufs[o].at[coords[a3], coords[a2], c, r]
        if phase == 1:
            return bufs[o].at[coords[a3], c, pl.ds(2 * half, 2)]
        return bufs[o].at[c, pl.ds(2 * half, 2)]

    starts = (0, K_CUTS[0] + V_CUTS[0], 2 * hd - K_CUTS[2] - V_CUTS[2])

    def copy(o, phase, c, half, step, idx):
        ref = part(o, phase, c, half)
        src = ref
        if phase == 0 and idx < 4:
            src = kv_ref.at[pl.ds(starts[o] + 48 * half, 48 if half == 0 else K_CUTS[o] + V_CUTS[o] - 48)]
        return pltpu.make_async_remote_copy(src, ref, send_sem.at[o, phase, idx], recv_sem.at[o, phase, idx], device_id=peer(ORDERS[o][phase], step), device_id_type=MESH)

    def recv(o, phase, c, half, step, idx):
        ref = part(o, phase, c, half)
        return pltpu.make_async_remote_copy(ref, ref, send_sem.at[o, phase, idx], recv_sem.at[o, phase, idx], device_id=peer(ORDERS[o][phase], step), device_id_type=MESH)

    sent = []

    def go(*args):
        cp = copy(*args)
        cp.start()
        sent.append(cp)

    for phase in range(3):
        for o in range(3):
            c = coords[ORDERS[o][phase]]
            go(o, phase, c, 0, 1, 0)
            go(o, phase, c, 1, -1, 1)
            go(o, phase, c, 1, 1, 2)
            go(o, phase, c, 0, -1, 3)
        for o in range(3):
            c = coords[ORDERS[o][phase]]
            left, right = lax.rem(c + 3, 4), lax.rem(c + 1, 4)
            recv(o, phase, left, 0, 1, 0).wait_recv()
            go(o, phase, left, 0, 1, 4)
            recv(o, phase, right, 1, -1, 1).wait_recv()
            go(o, phase, right, 1, -1, 5)
        if phase == 0:
            build_queries(q_ref, cuts_ref, q_ext, me * rows, heads, rows, hd)
            start_state(acc, m_ref, l_ref)
        for o in range(3):
            c = coords[ORDERS[o][phase]]
            left, right, far = lax.rem(c + 3, 4), lax.rem(c + 1, 4), lax.rem(c + 2, 4)
            recv(o, phase, left, 1, 1, 2).wait_recv()
            recv(o, phase, right, 0, -1, 3).wait_recv()
            recv(o, phase, far, 0, 1, 4).wait_recv()
            recv(o, phase, far, 1, -1, 5).wait_recv()

    q_base = me * rows

    def tile(t, causal):
        y, z = lax.rem(t, 4), t // 4
        ks, vs = [], []
        for x in range(4):
            pieces = (buf_a.at[z, y, x], buf_b.at[x, z, y], buf_c.at[y, x, z])
            for o in range(3):
                ks.append(pieces[o][0:K_CUTS[o], :])
            vs.append(jnp.concatenate([pieces[o][K_CUTS[o]:K_CUTS[o] + V_CUTS[o], :] for o in range(3)], axis=0))
        attend_tile(jnp.concatenate(ks, axis=0), jnp.concatenate(vs, axis=1), cuts_ref, q_ext, acc, m_ref, l_ref, t * 4 * rows, q_base, rows, causal, False)

    @pl.loop(0, me // 4)
    def _(t):
        tile(t, False)

    tile(me // 4, True)
    finish_state(mixed_ref, acc, l_ref, heads, rows, hd)
    for cp in sent:
        cp.wait_send()


GU = 512
NS = 4
OC = 512
DC = 256


def mlp_kernel(layer, next_layer, mixed_ref, x_ref, gm_ref, ga_ref, wo, wg, wu, wd, xout, nout, wo_b, wg_b, wu_b, wd_b, act, o_snd, o_rcv, d_snd, d_rcv, hid, nrm, wo_sem, wg_sem, wu_sem, wd_sem, send_sem, recv_sem):
    rows, model = x_ref.shape
    ff = wg.shape[2]
    full = ff // GU
    rest = ff - full * GU
    n_o = model // OC
    n_d = model // DC
    other = 1 - lax.axis_index("tp")

    def wo_copy(c):
        return pltpu.make_async_copy(wo.at[layer, :, pl.ds(c * OC, OC)], wo_b.at[c], wo_sem.at[c])

    def gu_copies(i, slot):
        off = pl.multiple_of(i * GU, GU)
        return (
            pltpu.make_async_copy(wg.at[layer, :, pl.ds(off, GU)], wg_b.at[slot], wg_sem.at[slot]),
            pltpu.make_async_copy(wu.at[layer, :, pl.ds(off, GU)], wu_b.at[slot], wu_sem.at[slot]),
        )

    rest_slot = full % NS

    def rest_copies():
        return (
            pltpu.make_async_copy(wg.at[layer, :, pl.ds(full * GU, rest)], wg_b.at[rest_slot, :, pl.ds(0, rest)], wg_sem.at[rest_slot]),
            pltpu.make_async_copy(wu.at[layer, :, pl.ds(full * GU, rest)], wu_b.at[rest_slot, :, pl.ds(0, rest)], wu_sem.at[rest_slot]),
        )

    def wd_copy(n):
        return pltpu.make_async_copy(wd.at[layer, :, pl.ds(pl.multiple_of(n * DC, DC), DC)], wd_b.at[n], wd_sem.at[n])

    for c in range(n_o):
        wo_copy(c).start()
    for i in range(NS):
        for cp in gu_copies(i, i):
            cp.start()

    barrier = pltpu.get_barrier_semaphore()
    pl.semaphore_signal(barrier, inc=1, device_id={"tp": other}, device_id_type=MESH)
    pl.semaphore_wait(barrier, 1)

    def o_send(c):
        return pltpu.make_async_remote_copy(o_snd.at[c], o_rcv.at[c], send_sem.at[c], recv_sem.at[c], device_id={"tp": other}, device_id_type=MESH)

    def d_send(n):
        return pltpu.make_async_remote_copy(d_snd.at[n], d_rcv.at[n], send_sem.at[n_o + n], recv_sem.at[n_o + n], device_id={"tp": other}, device_id_type=MESH)

    for c in range(n_o):
        wo_copy(c).wait()
        o_snd[c] = dot(mixed_ref[...], wo_b[c]).astype(BF16)
        o_send(c).start()
    sq = jnp.zeros((rows, 1), F32)
    for c in range(n_o):
        o_send(c).wait_recv()
        cols = slice(c * OC, (c + 1) * OC)
        out = (o_snd[c].astype(F32) + o_rcv[c].astype(F32)).astype(BF16)
        h = (x_ref[:, cols].astype(F32) + out.astype(F32)).astype(BF16)
        hid[:, cols] = h
        h = h.astype(F32)
        sq += jnp.sum(h * h, axis=1, keepdims=True)
    inv = lax.rsqrt(sq / model + EPS)
    for c in range(n_o):
        cols = slice(c * OC, (c + 1) * OC)
        nrm[:, cols] = (hid[:, cols].astype(F32) * inv * gm_ref[layer:layer + 1, cols].astype(F32)).astype(BF16)

    def gate_up(g_w, u_w):
        g = dot(nrm[...], g_w)
        u = dot(nrm[...], u_w)
        return (jax.nn.silu(g) * u).astype(BF16)

    @pl.loop(0, full)
    def _(i):
        slot = lax.rem(i, NS)
        for cp in gu_copies(i, slot):
            cp.wait()
        act[:, pl.ds(pl.multiple_of(i * GU, GU), GU)] = gate_up(wg_b[slot], wu_b[slot])

        @pl.when(i < full - NS)
        def _():
            for cp in gu_copies(i + NS, slot):
                cp.start()

        if rest:
            @pl.when(i == full - NS)
            def _():
                for cp in rest_copies():
                    cp.start()

        @pl.when(i < n_d)
        def _():
            wd_copy(i).start()

    if rest:
        for cp in rest_copies():
            cp.wait()
        act[:, full * GU:ff] = gate_up(wg_b[rest_slot, :, 0:rest], wu_b[rest_slot, :, 0:rest])

    @pl.loop(0, n_d)
    def _(n):
        wd_copy(n).wait()
        d_snd[n] = dot(act[...], wd_b[n]).astype(BF16)
        d_send(n).start()

    sq = jnp.zeros((rows, 1), F32)
    for n in range(n_d):
        d_send(n).wait_recv()
        cols = slice(n * DC, (n + 1) * DC)
        out = (d_snd[n].astype(F32) + d_rcv[n].astype(F32)).astype(BF16)
        h = (hid[:, cols].astype(F32) + out.astype(F32)).astype(BF16)
        xout[:, cols] = h
        h = h.astype(F32)
        sq += jnp.sum(h * h, axis=1, keepdims=True)
    inv = lax.rsqrt(sq / model + EPS)
    for n in range(n_d):
        cols = slice(n * DC, (n + 1) * DC)
        nout[:, cols] = (xout[:, cols].astype(F32) * inv * ga_ref[next_layer:next_layer + 1, cols].astype(F32)).astype(BF16)
    for c in range(n_o):
        o_send(c).wait_send()
    for n in range(n_d):
        d_send(n).wait_send()


VM = pl.BlockSpec(memory_space=pltpu.VMEM)
ANY = pl.BlockSpec(memory_space=pl.ANY)


def call_mlp(layer, next_layer, cid, mixed, x, g_mlp, g_attn, w_o, w_gate, w_up, w_down):
    rows, model = x.shape
    ff = w_gate.shape[2]
    depth = w_o.shape[1]
    n_o, n_d = model // OC, model // DC
    return pl.pallas_call(
        functools.partial(mlp_kernel, layer, next_layer),
        out_shape=[jax.ShapeDtypeStruct((rows, model), BF16)] * 2,
        in_specs=[VM] * 4 + [ANY] * 4,
        out_specs=[VM] * 2,
        scratch_shapes=[
            pltpu.VMEM((n_o, depth, OC), BF16),
            pltpu.VMEM((NS, model, GU), BF16),
            pltpu.VMEM((NS, model, GU), BF16),
            pltpu.VMEM((n_d, ff, DC), BF16),
            pltpu.VMEM((rows, ff), BF16),
            pltpu.VMEM((n_o, rows, OC), BF16),
            pltpu.VMEM((n_o, rows, OC), BF16),
            pltpu.VMEM((n_d, rows, DC), BF16),
            pltpu.VMEM((n_d, rows, DC), BF16),
            pltpu.VMEM((rows, model), BF16),
            pltpu.VMEM((rows, model), BF16),
            pltpu.SemaphoreType.DMA((n_o,)),
            pltpu.SemaphoreType.DMA((NS,)),
            pltpu.SemaphoreType.DMA((NS,)),
            pltpu.SemaphoreType.DMA((n_d,)),
            pltpu.SemaphoreType.DMA((n_o + n_d,)),
            pltpu.SemaphoreType.DMA((n_o + n_d,)),
        ],
        compiler_params=pltpu.CompilerParams(collective_id=cid, has_side_effects=True, vmem_limit_bytes=58 * 2**20),
        cost_estimate=pl.CostEstimate(flops=2 * rows * model * (3 * ff + depth), bytes_accessed=2 * model * (3 * ff + depth), transcendentals=0),
        name=f"mlp_{layer}",
    )(mixed, x, g_mlp, g_attn, w_o, w_gate, w_up, w_down)


def call_attention(windowed, cid, sp_size, q, kv, cuts):
    rows, width = q.shape
    hd = kv.shape[1]
    cols = width // hd * rows
    tail = [
        pltpu.VMEM((2 * hd, cols), BF16),
        pltpu.VMEM((hd, cols), F32),
        pltpu.VMEM((1, cols), F32),
        pltpu.VMEM((1, cols), F32),
    ]
    if windowed:
        back = WINDOW // rows
        body = functools.partial(window_kernel, sp_size, back)
        scratch = [pltpu.VMEM((back, 2 * rows, hd), BF16)] + tail + [pltpu.SemaphoreType.DMA((back,)), pltpu.SemaphoreType.DMA((back,))]
    else:
        body = global_kernel
        scratch = [pltpu.VMEM((4, 4, 4, a + b, hd), BF16) for a, b in zip(K_CUTS, V_CUTS)] + tail
        scratch += [pltpu.SemaphoreType.DMA((3, 3, 6)), pltpu.SemaphoreType.DMA((3, 3, 6)), pltpu.SemaphoreType.DMA]
    return pl.pallas_call(
        body,
        out_shape=jax.ShapeDtypeStruct((rows, width), BF16),
        in_specs=[VM] * 3,
        out_specs=VM,
        scratch_shapes=scratch,
        compiler_params=pltpu.CompilerParams(collective_id=cid, has_side_effects=True, vmem_limit_bytes=40 * 2**20),
        name="attn_w" if windowed else "attn_g",
    )(q, kv, cuts)


def solution(mesh):
    sp_size = mesh.shape["sp"]
    row_spec = P(("dp", "sp", "tp"), None)
    id_spec = P(("dp", "sp", "tp"))
    whole = P()
    in_specs = (row_spec, id_spec, id_spec, whole, P(None, None, "tp", None), whole, whole, P(None, "tp", None, None), whole, P(None, None, "tp"), P(None, None, "tp"), P(None, "tp", None))

    def local_fn(x, segment_ids, positions, g_attn, w_q, w_k, w_v, w_o, g_mlp, w_gate, w_up, w_down):
        tp_idx = lax.axis_index("tp")
        layers, model, heads_loc, head_dim = w_q.shape
        own_rows = x.shape[0]
        counts = jnp.stack([jnp.sum((segment_ids < 1).astype(jnp.int32)), jnp.sum((segment_ids < 2).astype(jnp.int32))])
        counts = lax.psum(counts, ("dp", "sp", "tp"))
        cuts = jnp.broadcast_to(jnp.pad(counts, (0, 6))[:, None], (8, head_dim))
        pos_shard = lax.all_gather(positions, "tp", tiled=True)
        cos_tab, sin_tab = rope_tables(pos_shard, head_dim)
        w_kv = jnp.concatenate([lax.dynamic_index_in_dim(w_k, tp_idx, 2, False), lax.dynamic_index_in_dim(w_v, tp_idx, 2, False)], axis=2)
        w_o2 = w_o.reshape(layers, heads_loc * head_dim, model)
        x = lax.all_gather(x, "tp", tiled=True)
        rows = x.shape[0]
        normed = rms_norm(x, g_attn[0])
        for layer in range(layers):
            windowed = layer % 2 == 0
            q = dot(normed, w_q[layer].reshape(model, heads_loc * head_dim)).astype(BF16)
            kv = dot(normed, w_kv[layer]).astype(BF16)
            q = rope(q.reshape(rows, heads_loc, head_dim), cos_tab, sin_tab).reshape(rows, heads_loc * head_dim)
            k = rope(kv[:, None, :head_dim], cos_tab, sin_tab).reshape(rows, head_dim)
            v_t = kv[:, head_dim:].T
            if windowed:
                kv = jnp.concatenate([k, v_t], axis=0)
            else:
                pieces, ko, vo = [], 0, 0
                for a, b in zip(K_CUTS, V_CUTS):
                    pieces += [k[ko:ko + a], v_t[vo:vo + b]]
                    ko, vo = ko + a, vo + b
                kv = jnp.concatenate(pieces, axis=0)
            mixed = call_attention(windowed, 10 if windowed else 11, sp_size, q, kv, cuts)
            x, normed = call_mlp(layer, (layer + 1) % layers, layer, mixed, x, g_mlp, g_attn, w_o2, w_gate, w_up, w_down)
        return lax.dynamic_slice_in_dim(x, tp_idx * own_rows, own_rows, 0)

    return jax.shard_map(local_fn, mesh=mesh, in_specs=in_specs, out_specs=row_spec, check_vma=False)
```

```python
import functools
import math

import jax
import jax.numpy as jnp
from jax import lax
from jax.experimental import pallas as pl
from jax.experimental.pallas import tpu as pltpu
from jax.sharding import PartitionSpec as P

EPS = 1e-6
ROPE_BASE = 10000.0
WINDOW = 1024
NEG = -1e30
MESH = pl.DeviceIdType.MESH
F32 = jnp.float32
BF16 = jnp.bfloat16
K_CUTS = (48, 48, 32)
V_CUTS = (32, 48, 48)
STRIDES = (1, 4, 16)
ORDERS = ((0, 1, 2), (1, 2, 0), (2, 0, 1))


def dot(a, b):
    return jnp.dot(a, b, preferred_element_type=F32)


def rope_tables(positions, head_dim):
    half_width = head_dim // 2
    inv_freq = ROPE_BASE ** (-jnp.arange(half_width, dtype=F32) / half_width)
    angles = positions.astype(F32)[:, None] * inv_freq[None, :]
    cos_tab, sin_tab = jnp.cos(angles), jnp.sin(angles)
    return jnp.concatenate([cos_tab, cos_tab], axis=1), jnp.concatenate([-sin_tab, sin_tab], axis=1)


def build_queries(q_ref, cuts_ref, q_ext, q_base, heads, rows, hd):
    for h in range(heads):
        q_ext[0:hd, h * rows:(h + 1) * rows] = q_ref[:, h * hd:(h + 1) * hd].astype(F32).T.astype(BF16)
    cut0 = cuts_ref[0:1, :]
    cut1 = cuts_ref[1:2, :]
    q_pos = q_base + lax.broadcasted_iota(jnp.int32, (hd, rows), 1)
    seg_q = (q_pos >= cut0).astype(jnp.int32) + (q_pos >= cut1).astype(jnp.int32)
    feat = lax.broadcasted_iota(jnp.int32, (hd, rows), 0)
    val = jnp.where((feat < 4) & (feat != seg_q), NEG, 0.0).astype(BF16)
    for h in range(heads):
        q_ext[hd:2 * hd, h * rows:(h + 1) * rows] = val


def key_features(cuts_ref, k_base, keys, hd):
    cut0 = cuts_ref[0:1, :]
    cut1 = cuts_ref[1:2, :]
    k_pos = k_base + lax.broadcasted_iota(jnp.int32, (keys, hd), 0)
    seg_k = (k_pos >= cut0).astype(jnp.int32) + (k_pos >= cut1).astype(jnp.int32)
    seg_k = jnp.where(k_pos < 0, 3, seg_k)
    feat = lax.broadcasted_iota(jnp.int32, (keys, hd), 1)
    return jnp.where(feat == seg_k, 1.0, 0.0).astype(BF16)


def attend_tile(k, v_t, cuts_ref, q_ext, acc, m_ref, l_ref, k_base, q_base, rows, causal, windowed):
    keys, hd = k.shape
    cols = q_ext.shape[1]
    feats = key_features(cuts_ref, k_base, keys, hd)
    k_ext = jnp.concatenate([k, feats], axis=1)
    scale = math.log2(math.e) * hd ** -0.5
    groups = [slice(g * COLS, (g + 1) * COLS) for g in range(cols // COLS)]
    bias = None
    if causal or windowed:
        k_pos = k_base + lax.broadcasted_iota(jnp.int32, (keys, rows), 0)
        q_pos = q_base + lax.broadcasted_iota(jnp.int32, (keys, rows), 1)
        ok = (k_pos <= q_pos) if causal else (q_pos - k_pos < WINDOW)
        bias = jnp.where(ok, 0.0, NEG)
        bias = jnp.concatenate([bias] * (COLS // rows), axis=1)
    scores = [dot(k_ext, q_ext[:, groups[0]])]
    for g, at in enumerate(groups):
        if g + 1 < len(groups):
            scores.append(dot(k_ext, q_ext[:, groups[g + 1]]))
        s = scores[g]
        if bias is not None:
            s = s + bias
        m_prev = m_ref[:, at]
        m_new = jnp.maximum(m_prev, jnp.max(s, axis=0, keepdims=True))
        p = jnp.exp2((s - m_new) * scale)
        alpha = jnp.exp2((m_prev - m_new) * scale)
        m_ref[:, at] = m_new
        l_ref[:, at] = l_ref[:, at] * alpha + jnp.sum(p, axis=0, keepdims=True)
        acc[:, at] = acc[:, at] * alpha + dot(v_t, p.astype(BF16))


def start_state(acc, m_ref, l_ref):
    acc[...] = jnp.zeros_like(acc)
    m_ref[...] = jnp.full_like(m_ref, -3e37)
    l_ref[...] = jnp.zeros_like(l_ref)


def finish_state(mixed_ref, acc, l_ref, heads, rows, hd):
    inv = 1.0 / l_ref[...]
    for h in range(heads):
        cols = slice(h * rows, (h + 1) * rows)
        mixed_ref[:, h * hd:(h + 1) * hd] = (acc[:, cols] * inv[:, cols]).T.astype(BF16)


def announce(peers, count):
    barrier = pltpu.get_barrier_semaphore()
    for peer in peers:
        pl.semaphore_signal(barrier, inc=1, device_id=peer, device_id_type=MESH)
    pl.semaphore_wait(barrier, count)


def window_attention(sp_size, back, q_ref, kv_ref, cuts_ref, mixed_ref, buf, q_ext, acc, m_ref, l_ref, send_sem, recv_sem):
    rows, width = q_ref.shape
    hd = kv_ref.shape[1]
    heads = width // hd
    me = lax.axis_index("sp")
    announce([{"tp": 1 - lax.axis_index("tp")}] + [{"sp": lax.rem(me - d + sp_size, sp_size)} for d in range(1, back + 1)], back + 1)
    copies = []
    for d in range(1, back + 1):
        cp = pltpu.make_async_remote_copy(kv_ref, buf.at[back - d], send_sem.at[d - 1], recv_sem.at[back - d], device_id={"sp": lax.rem(me + d, sp_size)}, device_id_type=MESH)
        cp.start()
        copies.append(cp)
    q_base = me * rows
    build_queries(q_ref, cuts_ref, q_ext, q_base, heads, rows, hd)
    start_state(acc, m_ref, l_ref)
    attend_tile(kv_ref[0:rows, :], kv_ref[rows:2 * rows, :], cuts_ref, q_ext, acc, m_ref, l_ref, q_base, q_base, rows, True, False)
    per = 4
    for t in reversed(range(back // per)):
        for j in range(per):
            slot = t * per + j
            copies[back - slot - 1].wait_recv()
        k = jnp.concatenate([buf[t * per + j, 0:rows, :] for j in range(per)], axis=0)
        v_t = jnp.concatenate([buf[t * per + j, rows:2 * rows, :] for j in range(per)], axis=1)
        attend_tile(k, v_t, cuts_ref, q_ext, acc, m_ref, l_ref, q_base + (t * per - back) * rows, q_base, rows, False, t == 0)
    finish_state(mixed_ref, acc, l_ref, heads, rows, hd)
    return copies


def global_attention(q_ref, kv_ref, cuts_ref, mixed_ref, buf_a, buf_b, buf_c, q_ext, acc, m_ref, l_ref, send_sem, recv_sem):
    rows, width = q_ref.shape
    hd = kv_ref.shape[1]
    heads = width // hd
    me = lax.axis_index("sp")
    coords = (lax.rem(me, 4), lax.rem(me // 4, 4), me // 16)
    bufs = (buf_a, buf_b, buf_c)

    def peer(axis, step):
        c = coords[axis]
        return {"sp": me + (lax.rem(c + step + 4, 4) - c) * STRIDES[axis]}

    offset = 0
    for o, (k_rows, v_rows) in enumerate(zip(K_CUTS, V_CUTS)):
        a1, a2, a3 = ORDERS[o]
        bufs[o][coords[a3], coords[a2], coords[a1]] = kv_ref[offset:offset + k_rows + v_rows, :]
        offset += k_rows + v_rows
    announce([{"tp": 1 - lax.axis_index("tp")}] + [peer(axis, step) for axis in range(3) for step in (1, -1)], 7)

    def part(o, phase, c, half):
        a1, a2, a3 = ORDERS[o]
        if phase == 0:
            cut = 48
            r = pl.ds(0, cut) if half == 0 else pl.ds(cut, K_CUTS[o] + V_CUTS[o] - cut)
            return bufs[o].at[coords[a3], coords[a2], c, r]
        if phase == 1:
            return bufs[o].at[coords[a3], c, pl.ds(2 * half, 2)]
        return bufs[o].at[c, pl.ds(2 * half, 2)]

    starts = (0, K_CUTS[0] + V_CUTS[0], 2 * hd - K_CUTS[2] - V_CUTS[2])

    def copy(o, phase, c, half, step, idx):
        ref = part(o, phase, c, half)
        src = ref
        if phase == 0 and idx < 4:
            src = kv_ref.at[pl.ds(starts[o] + 48 * half, 48 if half == 0 else K_CUTS[o] + V_CUTS[o] - 48)]
        return pltpu.make_async_remote_copy(src, ref, send_sem.at[o, phase, idx], recv_sem.at[o, phase, idx], device_id=peer(ORDERS[o][phase], step), device_id_type=MESH)

    def recv(o, phase, c, half, step, idx):
        ref = part(o, phase, c, half)
        return pltpu.make_async_remote_copy(ref, ref, send_sem.at[o, phase, idx], recv_sem.at[o, phase, idx], device_id=peer(ORDERS[o][phase], step), device_id_type=MESH)

    sent = []

    def go(*args):
        cp = copy(*args)
        cp.start()
        sent.append(cp)

    for phase in range(3):
        for o in range(3):
            c = coords[ORDERS[o][phase]]
            go(o, phase, c, 0, 1, 0)
            go(o, phase, c, 1, -1, 1)
            go(o, phase, c, 1, 1, 2)
            go(o, phase, c, 0, -1, 3)
        for o in range(3):
            c = coords[ORDERS[o][phase]]
            left, right = lax.rem(c + 3, 4), lax.rem(c + 1, 4)
            recv(o, phase, left, 0, 1, 0).wait_recv()
            go(o, phase, left, 0, 1, 4)
            recv(o, phase, right, 1, -1, 1).wait_recv()
            go(o, phase, right, 1, -1, 5)
        if phase == 0:
            build_queries(q_ref, cuts_ref, q_ext, me * rows, heads, rows, hd)
            start_state(acc, m_ref, l_ref)
        for o in range(3):
            c = coords[ORDERS[o][phase]]
            left, right, far = lax.rem(c + 3, 4), lax.rem(c + 1, 4), lax.rem(c + 2, 4)
            recv(o, phase, left, 1, 1, 2).wait_recv()
            recv(o, phase, right, 0, -1, 3).wait_recv()
            recv(o, phase, far, 0, 1, 4).wait_recv()
            recv(o, phase, far, 1, -1, 5).wait_recv()

    q_base = me * rows

    def tile(t, causal):
        y, z = lax.rem(t, 4), t // 4
        ks, vs = [], []
        for x in range(4):
            pieces = (buf_a.at[z, y, x], buf_b.at[x, z, y], buf_c.at[y, x, z])
            for o in range(3):
                ks.append(pieces[o][0:K_CUTS[o], :])
            vs.append(jnp.concatenate([pieces[o][K_CUTS[o]:K_CUTS[o] + V_CUTS[o], :] for o in range(3)], axis=0))
        attend_tile(jnp.concatenate(ks, axis=0), jnp.concatenate(vs, axis=1), cuts_ref, q_ext, acc, m_ref, l_ref, t * 4 * rows, q_base, rows, causal, False)

    @pl.loop(0, me // 4)
    def _(t):
        tile(t, False)

    tile(me // 4, True)
    finish_state(mixed_ref, acc, l_ref, heads, rows, hd)
    return sent


COLS = 256
GU = 512
NS = 4
OC = 512
DC = 256


def project(nrm, wq_chunks, w_kv, cos_ref, sin_ref, q_ref, kv_ref, windowed):
    rows = q_ref.shape[0]
    hd = kv_ref.shape[1]

    def rotate(t):
        t = t.astype(BF16).astype(F32)
        return (t * cos_ref[...] + pltpu.roll(t, hd // 2, 1) * sin_ref[...]).astype(BF16)

    kv = dot(nrm[...], w_kv)
    k = rotate(kv[:, 0:hd])
    v_t = kv[:, hd:2 * hd].astype(BF16).astype(F32).T.astype(BF16)
    if windowed:
        kv_ref[0:rows, :] = k
        kv_ref[rows:2 * rows, :] = v_t
    else:
        at, ko, vo = 0, 0, 0
        for a, b in zip(K_CUTS, V_CUTS):
            kv_ref[at:at + a, :] = k[ko:ko + a, :]
            kv_ref[at + a:at + a + b, :] = v_t[vo:vo + b, :]
            at, ko, vo = at + a + b, ko + a, vo + b
    col = 0
    for w in wq_chunks:
        q = dot(nrm[...], w())
        for h in range(q.shape[1] // hd):
            q_ref[:, col:col + hd] = rotate(q[:, h * hd:(h + 1) * hd])
            col += hd


def first_kernel(x_ref, ga_ref, cos_ref, sin_ref, cnt_ref, wq, wk, wv, q_out, kv_out, cuts_out, nrm, wq_b, wkv_b, tot, got, sems, send_sem, recv_sem):
    n_q = wq_b.shape[0]
    hd = wk.shape[3]
    tp = lax.axis_index("tp")
    cps = [pltpu.make_async_copy(w.at[0, tp], wkv_b.at[:, pl.ds(i * hd, hd)], sems.at[n_q + i]) for i, w in enumerate((wk, wv))]
    for c in range(n_q):
        cps.append(pltpu.make_async_copy(wq.at[0, :, pl.ds(c * GU, GU)], wq_b.at[c], sems.at[c]))
    for cp in cps:
        cp.start()
    me = lax.axis_index("sp")
    coords = (lax.rem(me, 4), lax.rem(me // 4, 4), me // 16)

    def peers(r):
        if r == 3:
            return [{"tp": 1 - lax.axis_index("tp")}]
        c = coords[r]
        return [{"sp": me + (lax.rem(c + step, 4) - c) * STRIDES[r]} for step in (1, 2, 3)]

    announce([peer for r in range(4) for peer in peers(r)], 10)
    tot[0] = cnt_ref[...]
    x = x_ref[...].astype(F32)
    inv = lax.rsqrt(jnp.mean(x * x, axis=1, keepdims=True) + EPS)
    nrm[...] = (x * inv * ga_ref[0:1, :].astype(F32)).astype(BF16)

    def send(r):
        return [pltpu.make_async_remote_copy(tot.at[r], got.at[r, j], send_sem.at[r, j], recv_sem.at[r, j], device_id=peer, device_id_type=MESH) for j, peer in enumerate(peers(r))]

    def take(r):
        total = tot[r]
        for j, cp in enumerate(send(r)):
            cp.wait_recv()
            total = total + got[r, j]
        if r < 3:
            tot[r + 1] = total
        else:
            cuts_out[...] = total

    for cp in send(0):
        cp.start()
    for cp in cps:
        cp.wait()
    take(0)
    for cp in send(1):
        cp.start()
    project(nrm, [lambda c=c: wq_b[c] for c in range(n_q)], wkv_b[...], cos_ref, sin_ref, q_out, kv_out, True)
    take(1)
    for r in (2, 3):
        for cp in send(r):
            cp.start()
        take(r)
    for r in range(4):
        for cp in send(r):
            cp.wait_send()


def layer_kernel(layer, last, sp_size, *refs):
    windowed = layer % 2 == 0
    q_ref, kv_ref, cuts_ref, x_ref, gm_ref, ga_ref, cos_ref, sin_ref, wo, wg, wu, wd, wq, wk, wv = refs[:15]
    refs = refs[15:]
    if last:
        xout, refs = refs[0], refs[1:]
        q_out = kv_out = None
    else:
        (xout, q_out, kv_out), refs = refs[:3], refs[3:]
    n_buf = 1 if windowed else 3
    bufs, refs = refs[:n_buf], refs[n_buf:]
    mixed_ref, q_ext, acc, m_ref, l_ref, a_send, a_recv = refs[:7]
    wo_b, wg_b, wu_b, wd_b, act, o_snd, o_rcv, d_snd, d_rcv, hid, nrm, wo_sem, wg_sem, wu_sem, wd_sem, send_sem, recv_sem = refs[7:]
    rows, model = x_ref.shape
    ff = wg.shape[2]
    full = ff // GU
    rest = ff - full * GU
    n_o = model // OC
    n_d = model // DC
    other = 1 - lax.axis_index("tp")

    def wo_copy(c):
        return pltpu.make_async_copy(wo.at[layer, :, pl.ds(c * OC, OC)], wo_b.at[c], wo_sem.at[c])

    def gu_copies(i, slot):
        off = pl.multiple_of(i * GU, GU)
        return (
            pltpu.make_async_copy(wg.at[layer, :, pl.ds(off, GU)], wg_b.at[slot], wg_sem.at[slot]),
            pltpu.make_async_copy(wu.at[layer, :, pl.ds(off, GU)], wu_b.at[slot], wu_sem.at[slot]),
        )

    rest_slot = full % NS

    def rest_copies():
        return (
            pltpu.make_async_copy(wg.at[layer, :, pl.ds(full * GU, rest)], wg_b.at[rest_slot, :, pl.ds(0, rest)], wg_sem.at[rest_slot]),
            pltpu.make_async_copy(wu.at[layer, :, pl.ds(full * GU, rest)], wu_b.at[rest_slot, :, pl.ds(0, rest)], wu_sem.at[rest_slot]),
        )

    def wd_copy(n):
        return pltpu.make_async_copy(wd.at[layer, :, pl.ds(pl.multiple_of(n * DC, DC), DC)], wd_b.at[n], wd_sem.at[n])

    for c in range(n_o):
        wo_copy(c).start()
    for i in range(NS):
        for cp in gu_copies(i, i):
            cp.start()

    for n in range(n_d):
        wd_copy(n).start()

    if windowed:
        sent = window_attention(sp_size, WINDOW // rows, q_ref, kv_ref, cuts_ref, mixed_ref, bufs[0], q_ext, acc, m_ref, l_ref, a_send, a_recv)
    else:
        sent = global_attention(q_ref, kv_ref, cuts_ref, mixed_ref, *bufs, q_ext, acc, m_ref, l_ref, a_send, a_recv)

    def o_send(c):
        return pltpu.make_async_remote_copy(o_snd.at[c], o_rcv.at[c], send_sem.at[c], recv_sem.at[c], device_id={"tp": other}, device_id_type=MESH)

    def d_send(n):
        return pltpu.make_async_remote_copy(d_snd.at[n], d_rcv.at[n], send_sem.at[n_o + n], recv_sem.at[n_o + n], device_id={"tp": other}, device_id_type=MESH)

    for c in range(n_o):
        wo_copy(c).wait()
        o_snd[c] = dot(mixed_ref[...], wo_b[c]).astype(BF16)
        o_send(c).start()
    sq = jnp.zeros((rows, 1), F32)
    for c in range(n_o):
        o_send(c).wait_recv()
        cols = slice(c * OC, (c + 1) * OC)
        out = (o_snd[c].astype(F32) + o_rcv[c].astype(F32)).astype(BF16)
        h = (x_ref[:, cols].astype(F32) + out.astype(F32)).astype(BF16)
        hid[:, cols] = h
        h = h.astype(F32)
        sq += jnp.sum(h * h, axis=1, keepdims=True)
    inv = lax.rsqrt(sq / model + EPS)
    for c in range(n_o):
        cols = slice(c * OC, (c + 1) * OC)
        nrm[:, cols] = (hid[:, cols].astype(F32) * inv * gm_ref[layer:layer + 1, cols].astype(F32)).astype(BF16)

    def gate_up(g_w, u_w):
        g = dot(nrm[...], g_w)
        u = dot(nrm[...], u_w)
        return (jax.nn.silu(g) * u).astype(BF16)

    @pl.loop(0, full)
    def _(i):
        slot = lax.rem(i, NS)
        for cp in gu_copies(i, slot):
            cp.wait()
        act[:, pl.ds(pl.multiple_of(i * GU, GU), GU)] = gate_up(wg_b[slot], wu_b[slot])

        @pl.when(i < full - NS)
        def _():
            for cp in gu_copies(i + NS, slot):
                cp.start()

        if rest:
            @pl.when(i == full - NS)
            def _():
                for cp in rest_copies():
                    cp.start()

    if rest:
        for cp in rest_copies():
            cp.wait()
        act[:, full * GU:ff] = gate_up(wg_b[rest_slot, :, 0:rest], wu_b[rest_slot, :, 0:rest])

    n_q = wq.shape[2] // GU
    next_copies = []
    if not last:
        for c in range(n_q):
            next_copies.append(pltpu.make_async_copy(wq.at[layer + 1, :, pl.ds(c * GU, GU)], wg_b.at[c], wg_sem.at[c]))
        for i, w in enumerate((wk, wv)):
            hd = w.shape[3]
            next_copies.append(pltpu.make_async_copy(w.at[layer + 1, 1 - other], wu_b.at[0, :, pl.ds(i * hd, hd)], wu_sem.at[i]))
    for cp in next_copies:
        cp.start()

    @pl.loop(0, n_d)
    def _(n):
        wd_copy(n).wait()
        d_snd[n] = dot(act[...], wd_b[n]).astype(BF16)
        d_send(n).start()

    sq = jnp.zeros((rows, 1), F32)
    for n in range(n_d):
        d_send(n).wait_recv()
        cols = slice(n * DC, (n + 1) * DC)
        out = (d_snd[n].astype(F32) + d_rcv[n].astype(F32)).astype(BF16)
        h = (hid[:, cols].astype(F32) + out.astype(F32)).astype(BF16)
        xout[:, cols] = h
        h = h.astype(F32)
        sq += jnp.sum(h * h, axis=1, keepdims=True)
    if not last:
        inv = lax.rsqrt(sq / model + EPS)
        for n in range(n_d):
            cols = slice(n * DC, (n + 1) * DC)
            nrm[:, cols] = (xout[:, cols].astype(F32) * inv * ga_ref[layer + 1:layer + 2, cols].astype(F32)).astype(BF16)
        for cp in next_copies:
            cp.wait()
        project(nrm, [lambda c=c: wg_b[c] for c in range(n_q)], wu_b[0, :, 0:2 * wk.shape[3]], cos_ref, sin_ref, q_out, kv_out, not windowed)
    for cp in sent:
        cp.wait_send()
    for c in range(n_o):
        o_send(c).wait_send()
    for n in range(n_d):
        d_send(n).wait_send()


VM = pl.BlockSpec(memory_space=pltpu.VMEM)
ANY = pl.BlockSpec(memory_space=pl.ANY)


def call_first(x, g_attn, cos_tab, sin_tab, counts, w_q, w_k, w_v):
    rows, model = x.shape
    width, hd = w_q.shape[2], w_k.shape[3]
    n_q = width // GU
    return pl.pallas_call(
        first_kernel,
        out_shape=[jax.ShapeDtypeStruct((rows, width), BF16), jax.ShapeDtypeStruct((2 * rows, hd), BF16), jax.ShapeDtypeStruct(counts.shape, jnp.int32)],
        in_specs=[VM] * 5 + [ANY] * 3,
        out_specs=[VM] * 3,
        scratch_shapes=[
            pltpu.VMEM((rows, model), BF16),
            pltpu.VMEM((n_q, model, GU), BF16),
            pltpu.VMEM((model, 2 * hd), BF16),
            pltpu.VMEM((4,) + counts.shape, jnp.int32),
            pltpu.VMEM((4, 3) + counts.shape, jnp.int32),
            pltpu.SemaphoreType.DMA((n_q + 2,)),
            pltpu.SemaphoreType.DMA((4, 3)),
            pltpu.SemaphoreType.DMA((4, 3)),
        ],
        compiler_params=pltpu.CompilerParams(collective_id=12, has_side_effects=True, vmem_limit_bytes=32 * 2**20),
        name="first",
    )(x, g_attn, cos_tab, sin_tab, counts, w_q, w_k, w_v)


def call_layer(layer, last, sp_size, q, kv, cuts, x, g_mlp, g_attn, cos_tab, sin_tab, w_o, w_gate, w_up, w_down, w_q, w_k, w_v):
    rows, model = x.shape
    ff = w_gate.shape[2]
    depth = w_o.shape[1]
    hd = kv.shape[1]
    width = q.shape[1]
    cols = width // hd * rows
    n_o, n_d = model // OC, model // DC
    out_shape = [jax.ShapeDtypeStruct((rows, model), BF16)]
    if not last:
        out_shape += [jax.ShapeDtypeStruct(q.shape, BF16), jax.ShapeDtypeStruct(kv.shape, BF16)]
    if layer % 2 == 0:
        back = WINDOW // rows
        scratch = [pltpu.VMEM((back, 2 * rows, hd), BF16)]
        sems = [pltpu.SemaphoreType.DMA((back,))] * 2
    else:
        scratch = [pltpu.VMEM((4, 4, 4, a + b, hd), BF16) for a, b in zip(K_CUTS, V_CUTS)]
        sems = [pltpu.SemaphoreType.DMA((3, 3, 6))] * 2
    scratch += [
        pltpu.VMEM((rows, width), BF16),
        pltpu.VMEM((2 * hd, cols), BF16),
        pltpu.VMEM((hd, cols), F32),
        pltpu.VMEM((1, cols), F32),
        pltpu.VMEM((1, cols), F32),
    ] + sems
    return pl.pallas_call(
        functools.partial(layer_kernel, layer, last, sp_size),
        out_shape=out_shape,
        in_specs=[VM] * 8 + [ANY] * 7,
        out_specs=[VM] * len(out_shape),
        scratch_shapes=scratch + [
            pltpu.VMEM((n_o, depth, OC), BF16),
            pltpu.VMEM((NS, model, GU), BF16),
            pltpu.VMEM((NS, model, GU), BF16),
            pltpu.VMEM((n_d, ff, DC), BF16),
            pltpu.VMEM((rows, ff), BF16),
            pltpu.VMEM((n_o, rows, OC), BF16),
            pltpu.VMEM((n_o, rows, OC), BF16),
            pltpu.VMEM((n_d, rows, DC), BF16),
            pltpu.VMEM((n_d, rows, DC), BF16),
            pltpu.VMEM((rows, model), BF16),
            pltpu.VMEM((rows, model), BF16),
            pltpu.SemaphoreType.DMA((n_o,)),
            pltpu.SemaphoreType.DMA((NS,)),
            pltpu.SemaphoreType.DMA((NS,)),
            pltpu.SemaphoreType.DMA((n_d,)),
            pltpu.SemaphoreType.DMA((n_o + n_d,)),
            pltpu.SemaphoreType.DMA((n_o + n_d,)),
        ],
        compiler_params=pltpu.CompilerParams(collective_id=layer, has_side_effects=True, vmem_limit_bytes=60 * 1024 * 1024),
        cost_estimate=pl.CostEstimate(flops=2 * rows * model * (3 * ff + 2 * depth), bytes_accessed=2 * model * (3 * ff + 2 * depth), transcendentals=0),
        name=f"layer_{layer}",
    )(q, kv, cuts, x, g_mlp, g_attn, cos_tab, sin_tab, w_o, w_gate, w_up, w_down, w_q, w_k, w_v)


def solution(mesh):
    sp_size = mesh.shape["sp"]
    row_spec = P(("dp", "sp", "tp"), None)
    id_spec = P(("dp", "sp", "tp"))
    whole = P()
    in_specs = (row_spec, id_spec, id_spec, whole, P(None, None, "tp", None), whole, whole, P(None, "tp", None, None), whole, P(None, None, "tp"), P(None, None, "tp"), P(None, "tp", None))

    def local_fn(x, segment_ids, positions, g_attn, w_q, w_k, w_v, w_o, g_mlp, w_gate, w_up, w_down):
        tp_idx = lax.axis_index("tp")
        layers, model, heads_loc, head_dim = w_q.shape
        own_rows = x.shape[0]
        counts = jnp.stack([jnp.sum((segment_ids < 1).astype(jnp.int32)), jnp.sum((segment_ids < 2).astype(jnp.int32))])
        counts = jnp.broadcast_to(jnp.pad(counts, (0, 6))[:, None], (8, head_dim))
        pos_shard = lax.all_gather(positions, "tp", tiled=True)
        cos_tab, sin_tab = rope_tables(pos_shard, head_dim)
        w_k2, w_v2 = w_k.transpose(0, 2, 1, 3), w_v.transpose(0, 2, 1, 3)
        w_o2 = w_o.reshape(layers, heads_loc * head_dim, model)
        w_q2 = w_q.reshape(layers, model, heads_loc * head_dim)
        x = lax.all_gather(x, "tp", tiled=True)
        q, kv, cuts = call_first(x, g_attn, cos_tab, sin_tab, counts, w_q2, w_k2, w_v2)
        for layer in range(layers):
            last = layer == layers - 1
            out = call_layer(layer, last, sp_size, q, kv, cuts, x, g_mlp, g_attn, cos_tab, sin_tab, w_o2, w_gate, w_up, w_down, w_q2, w_k2, w_v2)
            if last:
                x = out[0]
            else:
                x, q, kv = out
        return lax.dynamic_slice_in_dim(x, tp_idx * own_rows, own_rows, 0)

    return jax.shard_map(local_fn, mesh=mesh, in_specs=in_specs, out_specs=row_spec, check_vma=False)
```
